32 devices in a mesh: dp: 8 (over z, x), tp: 4 (over y, core).
Axes of the slice: x: 2, y: 2, z: 4, core: 2. Of those that a mesh axis runs over, the one named last changes fastest.
Arguments:
- hidden_in: bfloat16 [512, 3584], P(('dp', 'tp')), may hold values from -6 to 6
- query_latent: bfloat16 [512, 64, 512], P(('dp', 'tp')), may hold values from -348 to 347
- query_rope: bfloat16 [512, 4096], P(('dp', 'tp')), may hold values from -348 to 347
- cache_latent: bfloat16 [512, 128, 512], P(('dp', 'tp')), may hold values from -6 to 6
- cache_rope: bfloat16 [512, 64, 128], P(('dp', 'tp')), may hold values from -6 to 6
- lengths: int32 [512], P(('dp', 'tp')), may hold values from 16 to 128
- value_up: bfloat16 [512, 4096], P(None, 'tp'), may hold values from -1 to 1
- out_proj: bfloat16 [4096, 3584], P('tp'), may hold values from -0.09375 to 0.09375
- norm_gain: float32 [3584], replicated, may hold values from 0.1 to 1.9
- expert_gate: bfloat16 [32, 3584, 1024], P(('dp', 'tp')), may hold values from -0.09375 to 0.09375
- expert_down: bfloat16 [32, 1024, 3584], P(('dp', 'tp')), may hold values from -0.1875 to 0.1875
- expert_ids: int32 [512, 8], P(('dp', 'tp')), may hold values from 0 to 31, all different within a row; in each aligned block of 16 rows (0 to 15, 16 to 31, ...) at most 4 rows name the same one
- affinity: float32 [512, 8], P(('dp', 'tp')), may hold values from 0.05 to 1
Outputs:
- layer_out: bfloat16 [512, 3584], P(('dp', 'tp'))
The draws below stay inside these ranges and needn't reach their ends.
Inputs may be any that keep to these rules, and one draw needn't show every extreme that they name: `expert_ids`: in each aligned block of 16 rows (the rows of one device) no expert is named by more than 4 rows.
All inputs are finite; a program needn't handle non-finite values.
Results may differ from the reference program's by a relative error of at most 0.0081.
Values may be sent and summed in bfloat16 or wider, within the bound.
A program may use at most 128 MiB of HBM per device.

```python
import math
import jax
import jax.numpy as jnp
import numpy as np
from jax import lax

D = 3584
HEADS = 64
LAT = 512
ROPE = 64
HEAD_V = 64
FF = 1024
TOPK = 8
CTX = 128
TOK_DEV = 16
TOKENS = 512
EXPERTS = 32
CAP = 4


def key_parts(key):
    latent = jax.random.normal(jax.random.fold_in(key, 101), (TOKENS, CTX, LAT), jnp.float32)
    rotary = jax.random.normal(jax.random.fold_in(key, 102), (TOKENS, ROPE, CTX), jnp.float32)
    latent = jnp.clip(latent, -6.0, 6.0).astype(jnp.bfloat16).astype(jnp.float32)
    rotary = jnp.clip(rotary, -6.0, 6.0).astype(jnp.bfloat16).astype(jnp.float32)
    return (latent, rotary)


def draw_cache_latent(key, part):
    return key_parts(key)[0].astype(jnp.bfloat16)


def draw_cache_rope(key, part):
    return key_parts(key)[1].astype(jnp.bfloat16)


def query_parts(key):
    full_shape = (TOKENS, HEADS, LAT + ROPE)
    return jnp.clip(jax.random.normal(jax.random.fold_in(key, 103), full_shape, jnp.float32), -6.0, 6.0)


def draw_query_latent(key, part):
    return query_parts(key)[:, :, :LAT].astype(jnp.bfloat16)


def draw_query_rope(key, part):
    return query_parts(key)[:, :, LAT:].reshape(TOKENS, HEADS * ROPE).astype(jnp.bfloat16)


def plant(result, rng, smallest, high):
    spot = [jax.random.randint(jax.random.fold_in(rng, axis), (), 0, length) for axis, length in enumerate(result.shape)]
    main_axis = result.shape.index(max(result.shape))
    beside = spot[:main_axis] + [(spot[main_axis] + 1) % result.shape[main_axis]] + spot[main_axis + 1:]
    return result.at[tuple(spot)].set(smallest).at[tuple(beside)].set(high)


def shard_levels(own_key, extent, pieces, smallest, top_value):
    def one(axis_at, shards_of):
        draws = jax.random.uniform(jax.random.fold_in(jax.random.fold_in(own_key, 6), axis_at), (shards_of,), jnp.float32, smallest / len(pieces), top_value / len(pieces))
        return jnp.repeat(jnp.exp(draws), extent[axis_at] // shards_of).reshape((-1,) + (1,) * (len(extent) - axis_at - 1))

    level = one(*pieces[0])
    for cut in pieces[1:]:
        level = level * one(*cut)
    return level


def shared_out(key, own, number, rows, number_of, top, limit, slope):
    sequence = jax.random.permutation(key, number_of)
    heavy_load, common = load_shares(number_of, rows * top, limit, slope, True), load_shares(number_of, rows * top, limit, slope, False)
    places = jnp.arange(number_of)

    def named(tallies, rotation):
        used = int((tallies > 0).sum())
        fixed = max(1, used // 4)
        moved = fixed + (places - fixed + rotation * (used - fixed)) % max(1, number_of - fixed)
        return jnp.zeros((number_of,), jnp.int32).at[sequence[jnp.where(places < fixed, places, moved)]].set(jnp.asarray(tallies, jnp.int32))

    tallies = jnp.where(number % 4 == 0, named(heavy_load, number // 4), named(common, number - number // 4 - 1))
    mixed = jax.random.permutation(jax.random.fold_in(own, 3), number_of)
    source_of, receiver = mixed[0:number_of // 2 * 2:2], mixed[1:number_of // 2 * 2:2]
    room = jnp.minimum(tallies[source_of] - 1, limit - tallies[receiver]) // 2
    room = jnp.where((source_of == sequence[0]) | (receiver == sequence[0]) | (tallies[receiver] == 0), 0, jnp.maximum(room, 0))
    moved = jax.random.randint(jax.random.fold_in(own, 4), (number_of // 2,), 0, 1 << 20) % (room + 1)
    tallies = tallies.at[source_of].add(-moved).at[receiver].add(moved)
    labels = jnp.searchsorted(jnp.cumsum(tallies), jnp.arange(rows * top), side="right").astype(jnp.int32)
    grid = labels.reshape(top, rows).T
    grid = grid[jax.random.permutation(jax.random.fold_in(own, 1), rows)]
    rotation = jax.random.randint(jax.random.fold_in(own, 2), (rows, 1), 0, top)
    return jnp.take_along_axis(grid, (jnp.arange(top)[None, :] + rotation) % top, axis=1)


def load_shares(count, total, reach, slope, full):
    weights = [(1 << 20) // math.isqrt(standing ** slope) + 1 for standing in range(1, count + 1)]
    largest = reach if full else min(reach, max(-(-total // count), total * weights[0] // sum(weights)))
    least = 1 if total - largest >= count - 1 else 0
    given, surplus = [largest] + [least] * (count - 1), total - largest - least * (count - 1)
    while surplus > 0:
        free = [i for i in range(1, count) if given[i] < largest] or [i for i in range(1, count) if given[i] < reach]
        mass, remaining = sum([weights[i] for i in free]), surplus
        for i in free:
            addition = min(reach - given[i], max(1, remaining * weights[i] // mass), surplus)
            given[i] = given[i] + addition
            surplus = surplus - addition
    return np.array(given)


def gaussian(own_key, shape, width, limit, shards=(), kind=jnp.bfloat16):
    factor_of = shard_levels(own_key, shape, shards, -0.22, 0.18) if shards else 1.0
    values = jax.random.normal(own_key, shape, jnp.float32) * width * factor_of
    return jnp.minimum(jnp.maximum(values, -limit), limit).astype(kind)


def setup_inputs(seed: int = 0) -> dict:
    key_list = jax.random.split(jax.random.key(seed), 14)
    hidden_in = gaussian(key_list[0], (TOKENS, D), 1.0, 6.0, ((0, 32),))
    query_latent = draw_query_latent(jax.random.fold_in(key_list[13], 71), 0)
    query_rope = draw_query_rope(jax.random.fold_in(key_list[13], 71), 0)
    cache_latent = draw_cache_latent(jax.random.fold_in(key_list[13], 71), 0)
    cache_rope = draw_cache_rope(jax.random.fold_in(key_list[13], 71), 0)
    lengths = plant(jax.random.randint(key_list[5], (TOKENS,), CTX // 8, CTX + 1), jax.random.fold_in(key_list[5], 1), CTX // 8, CTX).astype(jnp.int32)
    value_up = gaussian(key_list[6], (LAT, HEADS * HEAD_V), (LAT // 16) ** -0.5, 1.0, ((1, 4),))
    out_proj = gaussian(key_list[7], (HEADS * HEAD_V, D), (HEADS * HEAD_V) ** -0.5, 0.09375, ((0, 4),))
    norm_gain = jnp.clip(1.0 + 0.18 * jax.random.normal(key_list[8], (D,), jnp.float32), 0.1, 1.9)
    expert_gate = gaussian(key_list[9], (EXPERTS, D, FF), D ** -0.5, 0.09375, ((0, 32),))
    expert_down = gaussian(key_list[10], (EXPERTS, FF, D), FF ** -0.5, 0.1875, ((0, 32),))
    expert_ids_keys = jax.random.split(jax.random.fold_in(key_list[11], 1), TOKENS // TOK_DEV)
    expert_ids_turns = jax.random.permutation(jax.random.fold_in(key_list[11], 3), TOKENS // TOK_DEV)
    expert_ids = jax.vmap(lambda own, number: shared_out(jax.random.fold_in(key_list[11], 2), own, number, TOK_DEV, EXPERTS, TOPK, CAP, 2))(expert_ids_keys, expert_ids_turns).reshape((TOKENS, TOPK))
    affinity = jnp.clip(jnp.exp(math.log(1.0) - 2.9957323 * jax.random.uniform(key_list[12], (TOKENS, TOPK), jnp.float32) ** shard_levels(key_list[12], (TOKENS, TOPK), ((0, 32),), -0.2, 0.2)), 0.05, 1.0)
    return dict(hidden_in=hidden_in, query_latent=query_latent, query_rope=query_rope, cache_latent=cache_latent, cache_rope=cache_rope, lengths=lengths, value_up=value_up, out_proj=out_proj, norm_gain=norm_gain, expert_gate=expert_gate, expert_down=expert_down, expert_ids=expert_ids, affinity=affinity)


score_scale = 192.0 ** (-0.5)
norm_eps = 1e-06
route_scale = 2.5

def attend(query_latent, query_rope, cache_latent, cache_rope, lengths):
    token_count, head_count, latent_width = query_latent.shape
    rope_width = cache_rope.shape[1]
    context = cache_latent.shape[1]
    latent_wide = cache_latent.astype(jnp.float32)
    query_rot = query_rope.astype(jnp.float32).reshape(token_count, head_count, rope_width)
    scores = jnp.einsum('thl,tpl->thp', query_latent.astype(jnp.float32), latent_wide)
    scores = scores + jnp.einsum('thr,trp->thp', query_rot, cache_rope.astype(jnp.float32))
    scores = scores * score_scale
    position = lax.broadcasted_iota(jnp.int32, (token_count, 1, context), 2)
    scores = jnp.where(position < lengths.astype(jnp.int32)[:, None, None], scores, -jnp.inf)
    row_max = lax.optimization_barrier(jnp.max(scores, axis=2, keepdims=True))
    raised = jnp.exp(scores - row_max)
    attn_weights = (raised / lax.optimization_barrier(jnp.sum(raised, axis=2, keepdims=True))).astype(jnp.bfloat16)
    latent_out = jnp.einsum('thp,tpl->thl', attn_weights.astype(jnp.float32), latent_wide)
    return latent_out.astype(jnp.bfloat16)

def reference(hidden_in, query_latent, query_rope, cache_latent, cache_rope, lengths, value_up, out_proj, norm_gain, expert_gate, expert_down, expert_ids, affinity):
    latent_out = attend(query_latent, query_rope, cache_latent, cache_rope, lengths)
    up_table = value_up.astype(jnp.float32).reshape(LAT, HEADS, HEAD_V)
    per_head = jnp.einsum('thl,lhv->thv', latent_out.astype(jnp.float32), up_table).astype(jnp.bfloat16)
    attn_sum = jnp.dot(per_head.reshape(TOKENS, HEADS * HEAD_V), out_proj, preferred_element_type=jnp.float32)
    hidden = (hidden_in.astype(jnp.float32) + attn_sum).astype(jnp.bfloat16)
    wide_hidden = hidden.astype(jnp.float32)
    inv_norm = lax.rsqrt(lax.optimization_barrier(jnp.mean(wide_hidden * wide_hidden, axis=1, keepdims=True)) + norm_eps)
    normed = (wide_hidden * inv_norm * norm_gain.astype(jnp.float32)).astype(jnp.bfloat16)
    blocks = TOKENS // TOK_DEV
    per_block = TOK_DEV * TOPK
    block_ids = expert_ids.astype(jnp.int32).reshape(blocks, per_block)
    expert_iota = jnp.arange(EXPERTS, dtype=jnp.int32)
    one_hot = (block_ids[:, :, None] == expert_iota[None, None, :]).astype(jnp.int32)
    earlier = jnp.cumsum(one_hot, axis=1) - one_hot
    slot_index = lax.optimization_barrier(jnp.sum(earlier * one_hot, axis=2)).astype(jnp.int32)
    block_number = jnp.arange(blocks, dtype=jnp.int32)[:, None]
    target = (block_ids * (blocks * CAP) + block_number * CAP + slot_index).reshape(-1)
    owner_row = jnp.arange(TOKENS * TOPK, dtype=jnp.int32) // TOPK
    route_weight = route_scale * affinity / lax.optimization_barrier(jnp.sum(affinity, axis=1, keepdims=True))
    source_row = jnp.full((EXPERTS * blocks * CAP,), TOKENS, jnp.int32).at[target].set(owner_row)
    row_weight = jnp.zeros((EXPERTS * blocks * CAP,), jnp.float32).at[target].set(route_weight.reshape(-1))
    padded = jnp.concatenate([normed, jnp.zeros((1, D), jnp.bfloat16)], axis=0)

    def one_expert(total, inputs):
        rows_here, weights_here, gate_here, down_here = inputs
        inner_act = jax.nn.silu(jnp.dot(padded[rows_here], gate_here, preferred_element_type=jnp.float32)).astype(jnp.bfloat16)
        answer = jnp.dot(inner_act, down_here, preferred_element_type=jnp.float32).astype(jnp.bfloat16).astype(jnp.float32)
        return (total.at[rows_here].add(weights_here[:, None] * answer, mode='drop'), None)
    moe_sum = lax.scan(one_expert, jnp.zeros((TOKENS, D), jnp.float32), (source_row.reshape(EXPERTS, -1), row_weight.reshape(EXPERTS, -1), expert_gate, expert_down))[0]
    return (wide_hidden + moe_sum).astype(jnp.bfloat16)
```

```python
import functools

import jax
import jax.numpy as jnp
from jax import lax
from jax.experimental import pallas as pl
from jax.experimental.pallas import tpu as pltpu
from jax.sharding import PartitionSpec as P

score_scale = 192.0 ** (-0.5)
norm_eps = 1e-06
route_scale = 2.5


def coordinates(axes, index):
    found = {}
    for name in reversed(axes):
        size = lax.axis_size(name)
        found[name] = lax.rem(index, size)
        index = lax.div(index, size)
    return found


def flat_index(axes):
    index = jnp.int32(0)
    for name in axes:
        index = index * lax.axis_size(name) + lax.axis_index(name)
    return index


def exchange_kernel(axes, count, block_ref, out_ref, send_sem, recv_sem, own_sem):
    me = flat_index(axes)
    barrier = pltpu.get_barrier_semaphore()
    peers = [coordinates(axes, lax.rem(me + step, count)) for step in range(1, count)]
    for peer in peers:
        pl.semaphore_signal(barrier, inc=1, device_id=peer, device_id_type=pl.DeviceIdType.MESH)
    own = pltpu.make_async_copy(block_ref.at[me], out_ref.at[me], own_sem)
    own.start()
    pl.semaphore_wait(barrier, count - 1)
    copies = []
    for step in range(1, count):
        copies.append(
            pltpu.make_async_remote_copy(
                src_ref=block_ref.at[lax.rem(me + step, count)],
                dst_ref=out_ref.at[me],
                send_sem=send_sem.at[step - 1],
                recv_sem=recv_sem.at[step - 1],
                device_id=peers[step - 1],
                device_id_type=pl.DeviceIdType.MESH,
            )
        )
        copies[-1].start()
    own.wait()
    for copy in copies:
        copy.wait()


def exchange(blocks, axes, collective_id):
    count = blocks.shape[0]
    return pl.pallas_call(
        functools.partial(exchange_kernel, axes, count),
        out_shape=jax.ShapeDtypeStruct(blocks.shape, blocks.dtype),
        in_specs=[pl.BlockSpec(memory_space=pltpu.VMEM)],
        out_specs=pl.BlockSpec(memory_space=pltpu.VMEM),
        scratch_shapes=[
            pltpu.SemaphoreType.DMA((count - 1,)),
            pltpu.SemaphoreType.DMA((count - 1,)),
            pltpu.SemaphoreType.DMA,
        ],
        compiler_params=pltpu.CompilerParams(collective_id=collective_id, has_side_effects=True),
    )(blocks)


def attend(query_latent, query_rope, cache_latent, cache_rope, lengths):
    token_count, head_count, latent_width = query_latent.shape
    rope_width = cache_rope.shape[1]
    context = cache_latent.shape[1]
    query_rot = query_rope.reshape(token_count, head_count, rope_width)
    scores = jnp.einsum(
        "thl,tpl->thp", query_latent, cache_latent, preferred_element_type=jnp.float32
    )
    scores = scores + jnp.einsum(
        "thr,trp->thp", query_rot, cache_rope, preferred_element_type=jnp.float32
    )
    scores = scores * score_scale
    position = lax.broadcasted_iota(jnp.int32, (token_count, 1, context), 2)
    scores = jnp.where(position < lengths[:, None, None], scores, -jnp.inf)
    row_max = jnp.max(scores, axis=2, keepdims=True)
    raised = jnp.exp(scores - row_max)
    attn_weights = (raised / jnp.sum(raised, axis=2, keepdims=True)).astype(jnp.bfloat16)
    latent_out = jnp.einsum(
        "thp,tpl->thl", attn_weights, cache_latent, preferred_element_type=jnp.float32
    )
    return latent_out.astype(jnp.bfloat16)


def per_device(
    hidden_in,
    query_latent,
    query_rope,
    cache_latent,
    cache_rope,
    lengths,
    value_up,
    out_proj,
    norm_gain,
    expert_gate,
    expert_down,
    expert_ids,
    affinity,
):
    latent_out = attend(query_latent, query_rope, cache_latent, cache_rope, lengths)
    group_size = lax.axis_size("tp")
    local_heads = latent_out.shape[1] // group_size
    tok_rows, head_count, latent_width = latent_out.shape
    grouped = latent_out.reshape(tok_rows, group_size, local_heads, latent_width).transpose(1, 0, 2, 3)
    by_heads = exchange(grouped, ("tp",), 0).reshape(-1, local_heads, latent_width)
    head_width = value_up.shape[1] // local_heads
    up_table = value_up.reshape(value_up.shape[0], local_heads, head_width)
    per_head = jnp.einsum(
        "thl,lhv->thv", by_heads, up_table, preferred_element_type=jnp.float32
    ).astype(jnp.bfloat16)
    partial = jnp.dot(
        per_head.reshape(group_size * tok_rows, local_heads * head_width),
        out_proj,
        preferred_element_type=jnp.float32,
    ).astype(jnp.bfloat16)
    partials = exchange(partial.reshape(group_size, tok_rows, -1), ("tp",), 1)
    attn_sum = jnp.sum(partials.astype(jnp.float32), axis=0)
    hidden = (hidden_in.astype(jnp.float32) + attn_sum).astype(jnp.bfloat16)
    wide_hidden = hidden.astype(jnp.float32)
    inv_norm = lax.rsqrt(jnp.mean(wide_hidden * wide_hidden, axis=1, keepdims=True) + norm_eps)
    normed = (wide_hidden * inv_norm * norm_gain).astype(jnp.bfloat16)
    tok_rows, top_count = expert_ids.shape
    width = normed.shape[1]
    experts = expert_gate.shape[0] * lax.axis_size("dp") * lax.axis_size("tp")
    capacity = max(2, -(-(tok_rows * top_count) // experts))
    flat_ids = expert_ids.reshape(-1)
    expert_iota = lax.broadcasted_iota(jnp.int32, (1, experts), 1)
    one_hot = (flat_ids[:, None] == expert_iota).astype(jnp.int32)
    earlier = jnp.cumsum(one_hot, axis=0) - one_hot
    slot_index = jnp.sum(earlier * one_hot, axis=1)
    target = flat_ids * capacity + slot_index
    owner_row = jnp.arange(tok_rows * top_count, dtype=jnp.int32) // top_count
    source_row = jnp.full((experts * capacity,), tok_rows, jnp.int32).at[target].set(owner_row)
    padded = jnp.concatenate([normed, jnp.zeros((1, width), jnp.bfloat16)], axis=0)
    outgoing = padded[source_row].reshape(experts, capacity, width)
    gate_local = expert_gate[0]
    down_local = expert_down[0]
    slot_rows = exchange(outgoing, ("dp", "tp"), 2)
    lead_shape = slot_rows.shape[:-1]
    flat_rows = slot_rows.reshape(-1, width)
    inner_act = jax.nn.silu(
        jnp.dot(flat_rows, gate_local, preferred_element_type=jnp.float32)
    ).astype(jnp.bfloat16)
    answer = jnp.dot(inner_act, down_local, preferred_element_type=jnp.float32).astype(jnp.bfloat16)
    answered = answer.reshape(lead_shape + (width,))
    returned = exchange(answered, ("dp", "tp"), 3)
    returned = returned.reshape(experts * capacity, width)
    picked = returned[target].reshape(tok_rows, top_count, width).astype(jnp.float32)
    route_weight = route_scale * affinity / jnp.sum(affinity, axis=1, keepdims=True)
    moe_sum = jnp.sum(picked * route_weight[:, :, None], axis=1)
    return (wide_hidden + moe_sum).astype(jnp.bfloat16)


def solution(mesh):
    return jax.shard_map(
        per_device,
        mesh=mesh,
        in_specs=(
            P(("dp", "tp"), None),
            P(("dp", "tp"), None, None),
            P(("dp", "tp"), None),
            P(("dp", "tp"), None, None),
            P(("dp", "tp"), None, None),
            P(("dp", "tp")),
            P(None, "tp"),
            P("tp", None),
            P(),
            P(("dp", "tp"), None, None),
            P(("dp", "tp"), None, None),
            P(("dp", "tp"), None),
            P(("dp", "tp"), None),
        ),
        out_specs=P(("dp", "tp"), None),
        check_vma=False,
    )
```

```python
import functools

import jax
import jax.numpy as jnp
from jax import lax
from jax.experimental import pallas as pl
from jax.experimental.pallas import tpu as pltpu
from jax.sharding import PartitionSpec as P

score_scale = 192.0 ** (-0.5)
norm_eps = 1e-06
route_scale = 2.5


def coordinates(axes, index):
    found = {}
    for name in reversed(axes):
        size = lax.axis_size(name)
        found[name] = lax.rem(index, size)
        index = lax.div(index, size)
    return found


def flat_index(axes):
    index = jnp.int32(0)
    for name in axes:
        index = index * lax.axis_size(name) + lax.axis_index(name)
    return index


def exchange_kernel(axes, count, block_ref, out_ref, send_sem, recv_sem, own_sem):
    me = flat_index(axes)
    barrier = pltpu.get_barrier_semaphore()
    peers = [coordinates(axes, lax.rem(me + step, count)) for step in range(1, count)]
    for peer in peers:
        pl.semaphore_signal(barrier, inc=1, device_id=peer, device_id_type=pl.DeviceIdType.MESH)
    own = pltpu.make_async_copy(block_ref.at[me], out_ref.at[me], own_sem)
    own.start()
    pl.semaphore_wait(barrier, count - 1)
    copies = []
    for step in range(1, count):
        copies.append(
            pltpu.make_async_remote_copy(
                src_ref=block_ref.at[lax.rem(me + step, count)],
                dst_ref=out_ref.at[me],
                send_sem=send_sem.at[step - 1],
                recv_sem=recv_sem.at[step - 1],
                device_id=peers[step - 1],
                device_id_type=pl.DeviceIdType.MESH,
            )
        )
        copies[-1].start()
    own.wait()
    for copy in copies:
        copy.wait()


def exchange(blocks, axes, collective_id):
    count = blocks.shape[0]
    return pl.pallas_call(
        functools.partial(exchange_kernel, axes, count),
        out_shape=jax.ShapeDtypeStruct(blocks.shape, blocks.dtype),
        in_specs=[pl.BlockSpec(memory_space=pltpu.VMEM)],
        out_specs=pl.BlockSpec(memory_space=pltpu.VMEM),
        scratch_shapes=[
            pltpu.SemaphoreType.DMA((count - 1,)),
            pltpu.SemaphoreType.DMA((count - 1,)),
            pltpu.SemaphoreType.DMA,
        ],
        compiler_params=pltpu.CompilerParams(collective_id=collective_id, has_side_effects=True),
    )(blocks)


def attend(query_latent, query_rope, cache_latent, cache_rope, lengths):
    token_count, head_count, latent_width = query_latent.shape
    rope_width = cache_rope.shape[1]
    context = cache_latent.shape[1]
    query_rot = query_rope.reshape(token_count, head_count, rope_width)
    scores = jnp.einsum(
        "thl,tpl->thp", query_latent, cache_latent, preferred_element_type=jnp.float32
    )
    scores = scores + jnp.einsum(
        "thr,trp->thp", query_rot, cache_rope, preferred_element_type=jnp.float32
    )
    scores = scores * score_scale
    position = lax.broadcasted_iota(jnp.int32, (token_count, 1, context), 2)
    scores = jnp.where(position < lengths[:, None, None], scores, -jnp.inf)
    row_max = jnp.max(scores, axis=2, keepdims=True)
    raised = jnp.exp(scores - row_max)
    attn_weights = (raised / jnp.sum(raised, axis=2, keepdims=True)).astype(jnp.bfloat16)
    latent_out = jnp.einsum(
        "thp,tpl->thl", attn_weights, cache_latent, preferred_element_type=jnp.float32
    )
    return latent_out.astype(jnp.bfloat16)


def per_device(
    hidden_in,
    query_latent,
    query_rope,
    cache_latent,
    cache_rope,
    lengths,
    value_up,
    out_proj,
    norm_gain,
    expert_gate,
    expert_down,
    expert_ids,
    affinity,
):
    latent_out = attend(query_latent, query_rope, cache_latent, cache_rope, lengths)
    group_size = lax.axis_size("tp")
    local_heads = latent_out.shape[1] // group_size
    tok_rows, head_count, latent_width = latent_out.shape
    grouped = latent_out.reshape(tok_rows, group_size, local_heads, latent_width).transpose(1, 0, 2, 3)
    by_heads = exchange(grouped, ("tp",), 0).reshape(-1, local_heads, latent_width)
    head_width = value_up.shape[1] // local_heads
    up_table = value_up.reshape(value_up.shape[0], local_heads, head_width)
    per_head = jnp.einsum(
        "thl,lhv->thv", by_heads, up_table, preferred_element_type=jnp.float32
    ).astype(jnp.bfloat16)
    partial = jnp.dot(
        per_head.reshape(group_size * tok_rows, local_heads * head_width),
        out_proj,
        preferred_element_type=jnp.float32,
    ).astype(jnp.bfloat16)
    partials = exchange(partial.reshape(group_size, tok_rows, -1), ("tp",), 1)
    attn_sum = jnp.sum(partials.astype(jnp.float32), axis=0)
    hidden = (hidden_in.astype(jnp.float32) + attn_sum).astype(jnp.bfloat16)
    wide_hidden = hidden.astype(jnp.float32)
    inv_norm = lax.rsqrt(jnp.mean(wide_hidden * wide_hidden, axis=1, keepdims=True) + norm_eps)
    normed = (wide_hidden * inv_norm * norm_gain).astype(jnp.bfloat16)
    dp, tp = lax.axis_size("dp"), lax.axis_size("tp")
    inner_dp = 2 if dp % 2 == 0 else 1
    experts = expert_gate.shape[0] * dp * tp
    capacity = max(2, -(-expert_ids.size // experts))
    shape = (dp // inner_dp, inner_dp * tp, inner_dp, tp, capacity)
    route = routing(expert_ids, affinity, shape)
    return run_experts(normed, hidden, expert_gate, expert_down, route, shape)


def experts_kernel(
    shape, normed_ref, hidden_ref, route_ref, gate_hbm, down_hbm, out_ref,
    block, route, sending, received, rows, inner, answers, back, partial, parts,
    gate, down, weight_sem, far_send, far_recv, route_send, route_recv,
    near_send, near_recv, own_sem, back_send, back_recv, part_send, part_recv,
):
    outer, plane, inner_dp, tp, cap = shape
    toks, width = normed_ref.shape
    slots = plane * cap
    at = lax.axis_index("dp")
    level = lax.div(at, inner_dp)
    me = lax.rem(at, inner_dp) * tp + lax.axis_index("tp")
    chunk = 256
    gate_copy = pltpu.make_async_copy(gate_hbm.at[0], gate, weight_sem.at[0])
    down_copy = pltpu.make_async_copy(down_hbm.at[0], down, weight_sem.at[1])
    gate_copy.start()
    down_copy.start()

    def far(step):
        return {"dp": lax.rem(level + step, outer) * inner_dp + lax.rem(at, inner_dp), "tp": lax.axis_index("tp")}

    def near(index):
        return {"dp": level * inner_dp + lax.div(index, tp), "tp": lax.rem(index, tp)}

    def remote(src, dst, send, recv, device):
        return pltpu.make_async_remote_copy(
            src_ref=src, dst_ref=dst, send_sem=send, recv_sem=recv,
            device_id=device, device_id_type=pl.DeviceIdType.MESH,
        )

    barrier = pltpu.get_barrier_semaphore()
    for step in range(1, outer):
        pl.semaphore_signal(barrier, inc=1, device_id=far(step), device_id_type=pl.DeviceIdType.MESH)
    for step in range(1, plane):
        pl.semaphore_signal(
            barrier, inc=1, device_id=near(lax.rem(me + step, plane)), device_id_type=pl.DeviceIdType.MESH
        )
    pl.semaphore_wait(barrier, outer + plane - 2)

    started = []
    far_copies, route_copies = {}, {}
    for step in range(1, outer):
        target = lax.rem(level + step, outer)
        route_copies[step] = remote(
            route_ref.at[target], route.at[step], route_send.at[step], route_recv.at[step], far(step)
        )
        far_copies[step] = remote(normed_ref, block.at[step], far_send.at[step], far_recv.at[step], far(step))
        route_copies[step].start()
        far_copies[step].start()

    near_copies, own_copies = {}, {}
    for step in range(outer):
        if step:
            route_copies[step].wait_recv()
            far_copies[step].wait_recv()
            pick, tokens = route[step, :slots, :toks], block[step]
        else:
            pick, tokens = route_ref[level, :slots, :toks], normed_ref[...]
        picked = jnp.dot(pick, tokens, preferred_element_type=jnp.float32).astype(jnp.bfloat16)
        for index in range(plane):
            sending[step, index] = picked[index * cap:(index + 1) * cap]
        own_copies[step] = pltpu.make_async_copy(sending.at[step, me], received.at[me, step], own_sem.at[step])
        own_copies[step].start()
        for hop in range(1, plane):
            peer = lax.rem(me + hop, plane)
            near_copies[step, hop] = remote(
                sending.at[step, peer], received.at[me, step],
                near_send.at[step, hop], near_recv.at[step, hop], near(peer),
            )
            near_copies[step, hop].start()
    for step in range(outer):
        own_copies[step].wait()
        for hop in range(1, plane):
            near_copies[step, hop].wait_recv()

    for index in range(plane):
        for step in range(outer):
            first = (index * outer + step) * cap
            rows[first:first + cap, :] = received[index, step]
    gate_copy.wait()

    @pl.loop(0, inner.shape[1] // chunk)
    def _(j):
        columns = pl.ds(pl.multiple_of(j * chunk, chunk), chunk)
        pre = jnp.dot(rows[...], gate[:, columns], preferred_element_type=jnp.float32)
        inner[:, columns] = jax.nn.silu(pre).astype(jnp.bfloat16)

    down_copy.wait()

    @pl.loop(0, width // chunk)
    def _(j):
        columns = pl.ds(pl.multiple_of(j * chunk, chunk), chunk)
        answer = jnp.dot(inner[...], down[:, columns], preferred_element_type=jnp.float32).astype(jnp.bfloat16)
        for index in range(plane):
            for step in range(outer):
                first = (index * outer + step) * cap
                answers[step, index, :, columns] = answer[first:first + cap]

    back_copies, own_back = {}, {}
    order = list(range(1, outer)) + [0]
    for step in order:
        for hop in range(1, plane):
            peer = lax.rem(me + hop, plane)
            back_copies[step, hop] = remote(
                answers.at[step, peer], back.at[step, me],
                back_send.at[step, hop], back_recv.at[step, hop], near(peer),
            )
            back_copies[step, hop].start()
        own_back[step] = pltpu.make_async_copy(answers.at[step, me], back.at[step, me], own_sem.at[step])
        own_back[step].start()
    part_copies = {}
    total = hidden_ref[...].astype(jnp.float32)
    for step in order:
        own_back[step].wait()
        for hop in range(1, plane):
            back_copies[step, hop].wait_recv()
        arrived = jnp.concatenate([back[step, index] for index in range(plane)], axis=0)
        if step:
            high, low = route[step, slots:slots + toks, :slots], route[step, slots + toks:, :slots]
        else:
            high, low = route_ref[level, slots:slots + toks, :slots], route_ref[level, slots + toks:, :slots]
        mixed = jnp.dot(high, arrived, preferred_element_type=jnp.float32) + jnp.dot(
            low, arrived, preferred_element_type=jnp.float32
        )
        if step:
            partial[step] = mixed.astype(jnp.bfloat16)
            part_copies[step] = remote(
                partial.at[step], parts.at[step], part_send.at[step], part_recv.at[step], far(outer - step)
            )
            part_copies[step].start()
        else:
            total = total + mixed
    for step in range(1, outer):
        part_copies[step].wait_recv()
        total = total + parts[step].astype(jnp.float32)
    out_ref[...] = total.astype(jnp.bfloat16)
    for step in range(1, outer):
        route_copies[step].wait_send()
        far_copies[step].wait_send()
        part_copies[step].wait_send()
    for step in range(outer):
        for hop in range(1, plane):
            near_copies[step, hop].wait_send()
            back_copies[step, hop].wait_send()


def run_experts(normed, hidden, expert_gate, expert_down, route, shape):
    outer, plane, _, _, cap = shape
    toks, width = normed.shape
    ff = expert_gate.shape[2]
    count = outer * plane * cap
    dma = pltpu.SemaphoreType.DMA
    vmem = pl.BlockSpec(memory_space=pltpu.VMEM)
    hbm = pl.BlockSpec(memory_space=pl.ANY)
    low = jnp.bfloat16
    return pl.pallas_call(
        functools.partial(experts_kernel, shape),
        out_shape=jax.ShapeDtypeStruct((toks, width), low),
        in_specs=[vmem, vmem, vmem, hbm, hbm],
        out_specs=vmem,
        scratch_shapes=[
            pltpu.VMEM((outer, toks, width), low),
            pltpu.VMEM(route.shape, low),
            pltpu.VMEM((outer, plane, cap, width), low),
            pltpu.VMEM((plane, outer, cap, width), low),
            pltpu.VMEM((count, width), low),
            pltpu.VMEM((count, ff), low),
            pltpu.VMEM((outer, plane, cap, width), low),
            pltpu.VMEM((outer, plane, cap, width), low),
            pltpu.VMEM((outer, toks, width), low),
            pltpu.VMEM((outer, toks, width), low),
            pltpu.VMEM(expert_gate.shape[1:], low),
            pltpu.VMEM(expert_down.shape[1:], low),
            dma((2,)), dma((outer,)), dma((outer,)), dma((outer,)), dma((outer,)),
            dma((outer, plane)), dma((outer, plane)), dma((outer,)),
            dma((outer, plane)), dma((outer, plane)), dma((outer,)), dma((outer,)),
        ],
        compiler_params=pltpu.CompilerParams(
            collective_id=2, has_side_effects=True, vmem_limit_bytes=60 * 1024 * 1024
        ),
    )(normed, hidden, route, expert_gate, expert_down)


def routing(expert_ids, affinity, shape):
    outer, plane, _, _, cap = shape
    toks = expert_ids.shape[0]
    experts = outer * plane
    weight = route_scale * affinity / jnp.sum(affinity, axis=1, keepdims=True)
    named = expert_ids[:, :, None] == lax.broadcasted_iota(jnp.int32, (1, 1, experts), 2)
    chosen = jnp.sum(named.astype(jnp.int32), axis=1)
    weights = jnp.sum(jnp.where(named, weight[:, :, None], 0.0), axis=1)
    before = lax.broadcasted_iota(jnp.int32, (toks, toks, 1), 1) < lax.broadcasted_iota(
        jnp.int32, (toks, toks, 1), 0
    )
    rank = jnp.sum(jnp.where(before, chosen[None], 0), axis=1)
    rank = jnp.where(chosen > 0, rank, -1)
    in_slot = rank[:, :, None] == lax.broadcasted_iota(jnp.int32, (1, 1, cap), 2)
    in_slot = in_slot.reshape(toks, outer, plane * cap)
    spread = jnp.repeat(weights, cap, axis=1).reshape(toks, outer, plane * cap)
    spread = jnp.where(in_slot, spread, 0.0)
    high = spread.astype(jnp.bfloat16)
    rest = (spread - high.astype(jnp.float32)).astype(jnp.bfloat16)
    lanes = 128 * (-(-max(toks, plane * cap) // 128))

    def padded(array):
        return jnp.pad(array, ((0, 0), (0, 0), (0, lanes - array.shape[2])))

    pick = padded(in_slot.astype(jnp.bfloat16).transpose(1, 2, 0))
    return jnp.concatenate(
        [pick, padded(high.transpose(1, 0, 2)), padded(rest.transpose(1, 0, 2))], axis=1
    )


def solution(mesh):
    return jax.shard_map(
        per_device,
        mesh=mesh,
        in_specs=(
            P(("dp", "tp"), None),
            P(("dp", "tp"), None, None),
            P(("dp", "tp"), None),
            P(("dp", "tp"), None, None),
            P(("dp", "tp"), None, None),
            P(("dp", "tp")),
            P(None, "tp"),
            P("tp", None),
            P(),
            P(("dp", "tp"), None, None),
            P(("dp", "tp"), None, None),
            P(("dp", "tp"), None),
            P(("dp", "tp"), None),
        ),
        out_specs=P(("dp", "tp"), None),
        check_vma=False,
    )
```

```python
import functools

import jax
import jax.numpy as jnp
from jax import lax
from jax.experimental import pallas as pl
from jax.experimental.pallas import tpu as pltpu
from jax.sharding import PartitionSpec as P

score_scale = 192.0 ** (-0.5)
norm_eps = 1e-06
route_scale = 2.5


def attention_kernel(
    batch, tile, query_hbm, rot_ref, cache_hbm, rope_hbm, lengths_ref, hidden_in_hbm, gain_ref,
    up_hbm, proj_hbm, hidden_ref, normed_ref, leaving, arrived, heads, partial, parts, total, up, proj,
    query_ref, cache_ref, rope_ref, hidden_in_ref, weight_sem, input_sem, out_send, out_recv, part_send, part_recv,
):
    toks, head_count, latent = query_hbm.shape
    context = cache_ref.shape[1]
    group = leaving.shape[0]
    local = head_count // group
    width = proj.shape[1]
    me = lax.axis_index("tp")
    input_copies = []
    for number in range(toks // batch):
        span = pl.ds(number * batch, batch)
        pairs = ((query_hbm, query_ref), (cache_hbm, cache_ref), (rope_hbm, rope_ref))
        input_copies.append([
            pltpu.make_async_copy(src.at[span], dst.at[span], input_sem.at[number, index])
            for index, (src, dst) in enumerate(pairs)
        ])
        for copy in input_copies[-1]:
            copy.start()
    hidden_copy = pltpu.make_async_copy(hidden_in_hbm, hidden_in_ref, weight_sem.at[2])
    up_copy = pltpu.make_async_copy(up_hbm, up, weight_sem.at[0])
    proj_copy = pltpu.make_async_copy(proj_hbm, proj, weight_sem.at[1])
    up_copy.start()
    proj_copy.start()
    hidden_copy.start()
    peers = [lax.rem(me + step, group) for step in range(group)]
    barrier = pltpu.get_barrier_semaphore()
    for step in range(1, group):
        pl.semaphore_signal(
            barrier, inc=1, device_id={"tp": peers[step]}, device_id_type=pl.DeviceIdType.MESH
        )

    def remote(src, dst, send, recv, step):
        return pltpu.make_async_remote_copy(
            src_ref=src, dst_ref=dst, send_sem=send, recv_sem=recv,
            device_id={"tp": peers[step]}, device_id_type=pl.DeviceIdType.MESH,
        )

    position = lax.broadcasted_iota(jnp.int32, (head_count, context), 1)
    out_copies = {}
    for first in range(0, toks, batch):
        for copy in input_copies[first // batch]:
            copy.wait()
        scores = []
        for t in range(first, first + batch):
            score = lax.dot_general(
                query_ref[t], cache_ref[t], (((1,), (1,)), ((), ())), preferred_element_type=jnp.float32
            )
            score = score + jnp.dot(rot_ref[t], rope_ref[t], preferred_element_type=jnp.float32)
            scores.append(jnp.where(position < lengths_ref[t], score * score_scale, -jnp.inf))
        weights = []
        for score in scores:
            raised = jnp.exp(score - jnp.max(score, axis=1, keepdims=True))
            weights.append((raised / jnp.sum(raised, axis=1, keepdims=True)).astype(jnp.bfloat16))
        for offset, weight in enumerate(weights):
            t = first + offset
            mixed = jnp.dot(weight, cache_ref[t], preferred_element_type=jnp.float32).astype(jnp.bfloat16)
            for part in range(group):
                leaving[part, t] = mixed[part * local:(part + 1) * local]
        if first == 0:
            pl.semaphore_wait(barrier, group - 1)
        span = pl.ds(first, batch)
        for step in range(1, group):
            number = first // batch
            out_copies[number, step] = remote(
                leaving.at[peers[step], span], arrived.at[step, span],
                out_send.at[number, step], out_recv.at[number, step], step,
            )
            out_copies[number, step].start()

    up_copy.wait()
    head_width = up.shape[1] // local
    lane = lax.broadcasted_iota(jnp.int32, (local, up.shape[1]), 1)
    row = lax.broadcasted_iota(jnp.int32, (local, up.shape[1]), 0)
    own_head = lax.div(lane, head_width) == row
    for step in range(group):
        for first in range(0, toks, batch):
            if step:
                out_copies[first // batch, step].wait_recv()
        source = leaving[me] if step == 0 else arrived[step]
        flat = source.reshape(toks * local, latent)
        for column in range(0, up.shape[1], 256):
            wide = jnp.dot(flat, up[:, column:column + 256], preferred_element_type=jnp.float32)
            wide = wide.reshape(toks, local, 256)
            kept = jnp.where(own_head[None, :, column:column + 256], wide, 0.0)
            heads[step * toks:(step + 1) * toks, column:column + 256] = jnp.sum(kept, axis=1).astype(jnp.bfloat16)
    proj_copy.wait()
    part_copies = {}
    for number in range(width // tile):
        columns = slice(number * tile, (number + 1) * tile)
        product = jnp.dot(heads[...], proj[:, columns], preferred_element_type=jnp.float32)
        total[:, columns] = product[:toks]
        for step in range(1, group):
            partial[number, step] = product[step * toks:(step + 1) * toks].astype(jnp.bfloat16)
            back = group - step
            part_copies[number, step] = remote(
                partial.at[number, step], parts.at[number, step],
                part_send.at[number, step], part_recv.at[number, step], back,
            )
            part_copies[number, step].start()
    hidden_copy.wait()
    squares = jnp.zeros((toks, 1), jnp.float32)
    for number in range(width // tile):
        columns = slice(number * tile, (number + 1) * tile)
        value = total[:, columns]
        for step in range(1, group):
            part_copies[number, step].wait_recv()
            value = value + parts[number, step].astype(jnp.float32)
        low = (hidden_in_ref[:, columns].astype(jnp.float32) + value).astype(jnp.bfloat16)
        hidden_ref[:, columns] = low
        squares = squares + jnp.sum(low.astype(jnp.float32) * low.astype(jnp.float32), axis=1, keepdims=True)
    inv_norm = lax.rsqrt(squares / width + norm_eps)
    normed_ref[...] = (hidden_ref[...].astype(jnp.float32) * inv_norm * gain_ref[...]).astype(jnp.bfloat16)
    for copy in list(out_copies.values()) + list(part_copies.values()):
        copy.wait_send()


def run_attention(query, rot, cache, rope, lengths, hidden_in, gain, value_up, out_proj):
    toks, head_count, latent = query.shape
    group = lax.axis_size("tp")
    local = head_count // group
    width = out_proj.shape[1]
    batch = 4 if toks % 4 == 0 else 1
    tile = 512 if width % 512 == 0 else 128
    tiles = width // tile
    dma = pltpu.SemaphoreType.DMA
    vmem = pl.BlockSpec(memory_space=pltpu.VMEM)
    hbm = pl.BlockSpec(memory_space=pl.ANY)
    smem = pl.BlockSpec(memory_space=pltpu.SMEM)
    low = jnp.bfloat16
    return pl.pallas_call(
        functools.partial(attention_kernel, batch, tile),
        out_shape=[jax.ShapeDtypeStruct((toks, width), low)] * 2,
        in_specs=[hbm, vmem, hbm, hbm, smem, hbm, vmem, hbm, hbm],
        out_specs=[vmem, vmem],
        scratch_shapes=[
            pltpu.VMEM((group, toks, local, latent), low),
            pltpu.VMEM((group, toks, local, latent), low),
            pltpu.VMEM((group * toks, out_proj.shape[0]), low),
            pltpu.VMEM((tiles, group, toks, tile), low),
            pltpu.VMEM((tiles, group, toks, tile), low),
            pltpu.VMEM((toks, width), jnp.float32),
            pltpu.VMEM(value_up.shape, low),
            pltpu.VMEM(out_proj.shape, low),
            pltpu.VMEM(query.shape, low),
            pltpu.VMEM(cache.shape, low),
            pltpu.VMEM(rope.shape, low),
            pltpu.VMEM(hidden_in.shape, low),
            dma((3,)), dma((toks // batch, 3)), dma((toks // batch, group)), dma((toks // batch, group)),
            dma((tiles, group)), dma((tiles, group)),
        ],
        compiler_params=pltpu.CompilerParams(
            collective_id=0, has_side_effects=True, vmem_limit_bytes=60 * 1024 * 1024
        ),
    )(query, rot, cache, rope, lengths, hidden_in, gain, value_up, out_proj)


def per_device(
    hidden_in,
    query_latent,
    query_rope,
    cache_latent,
    cache_rope,
    lengths,
    value_up,
    out_proj,
    norm_gain,
    expert_gate,
    expert_down,
    expert_ids,
    affinity,
):
    toks, head_count, _ = query_latent.shape
    hidden, normed = run_attention(
        query_latent, query_rope.reshape(toks, head_count, -1), cache_latent, cache_rope, lengths,
        hidden_in, norm_gain.reshape(1, -1), value_up, out_proj,
    )
    dp, tp = lax.axis_size("dp"), lax.axis_size("tp")
    inner_dp = 2 if dp % 2 == 0 else 1
    experts = expert_gate.shape[0] * dp * tp
    capacity = max(2, -(-expert_ids.size // experts))
    shape = (dp // inner_dp, inner_dp * tp, inner_dp, tp, capacity)
    route = routing(expert_ids, affinity, shape)
    return run_experts(normed, hidden, expert_gate, expert_down, route, shape)


def experts_kernel(
    shape, normed_ref, hidden_ref, route_ref, gate_hbm, down_hbm, out_ref,
    block, route, sending, received, rows, inner, answers, back, partial, parts,
    gate, down, weight_sem, far_send, far_recv, route_send, route_recv,
    near_send, near_recv, own_sem, back_send, back_recv, part_send, part_recv,
):
    outer, plane, inner_dp, tp, cap = shape
    toks, width = normed_ref.shape
    slots = plane * cap
    at = lax.axis_index("dp")
    level = lax.div(at, inner_dp)
    me = lax.rem(at, inner_dp) * tp + lax.axis_index("tp")
    chunk = 256
    gate_copy = pltpu.make_async_copy(gate_hbm.at[0], gate, weight_sem.at[0])
    down_copy = pltpu.make_async_copy(down_hbm.at[0], down, weight_sem.at[1])
    gate_copy.start()
    down_copy.start()

    def far(step):
        return {"dp": lax.rem(level + step, outer) * inner_dp + lax.rem(at, inner_dp), "tp": lax.axis_index("tp")}

    def near(index):
        return {"dp": level * inner_dp + lax.div(index, tp), "tp": lax.rem(index, tp)}

    def remote(src, dst, send, recv, device):
        return pltpu.make_async_remote_copy(
            src_ref=src, dst_ref=dst, send_sem=send, recv_sem=recv,
            device_id=device, device_id_type=pl.DeviceIdType.MESH,
        )

    barrier = pltpu.get_barrier_semaphore()
    for step in range(1, outer):
        pl.semaphore_signal(barrier, inc=1, device_id=far(step), device_id_type=pl.DeviceIdType.MESH)
    for step in range(1, plane):
        pl.semaphore_signal(
            barrier, inc=1, device_id=near(lax.rem(me + step, plane)), device_id_type=pl.DeviceIdType.MESH
        )
    pl.semaphore_wait(barrier, outer + plane - 2)

    started = []
    far_copies, route_copies = {}, {}
    for step in range(1, outer):
        target = lax.rem(level + step, outer)
        route_copies[step] = remote(
            route_ref.at[target], route.at[step], route_send.at[step], route_recv.at[step], far(step)
        )
        far_copies[step] = remote(normed_ref, block.at[step], far_send.at[step], far_recv.at[step], far(step))
        route_copies[step].start()
        far_copies[step].start()

    near_copies, own_copies = {}, {}
    for step in range(outer):
        if step:
            route_copies[step].wait_recv()
            far_copies[step].wait_recv()
            pick, tokens = route[step, :slots, :toks], block[step]
        else:
            pick, tokens = route_ref[level, :slots, :toks], normed_ref[...]
        picked = jnp.dot(pick, tokens, preferred_element_type=jnp.float32).astype(jnp.bfloat16)
        for index in range(plane):
            sending[step, index] = picked[index * cap:(index + 1) * cap]
        own_copies[step] = pltpu.make_async_copy(sending.at[step, me], received.at[me, step], own_sem.at[step])
        own_copies[step].start()
        for hop in range(1, plane):
            peer = lax.rem(me + hop, plane)
            near_copies[step, hop] = remote(
                sending.at[step, peer], received.at[me, step],
                near_send.at[step, hop], near_recv.at[step, hop], near(peer),
            )
            near_copies[step, hop].start()
    for step in range(outer):
        own_copies[step].wait()
        for hop in range(1, plane):
            near_copies[step, hop].wait_recv()

    for index in range(plane):
        for step in range(outer):
            first = (index * outer + step) * cap
            rows[first:first + cap, :] = received[index, step]
    gate_copy.wait()

    @pl.loop(0, inner.shape[1] // chunk)
    def _(j):
        columns = pl.ds(pl.multiple_of(j * chunk, chunk), chunk)
        pre = jnp.dot(rows[...], gate[:, columns], preferred_element_type=jnp.float32)
        inner[:, columns] = jax.nn.silu(pre).astype(jnp.bfloat16)

    down_copy.wait()

    @pl.loop(0, width // chunk)
    def _(j):
        columns = pl.ds(pl.multiple_of(j * chunk, chunk), chunk)
        answer = jnp.dot(inner[...], down[:, columns], preferred_element_type=jnp.float32).astype(jnp.bfloat16)
        for index in range(plane):
            for step in range(outer):
                first = (index * outer + step) * cap
                answers[step, index, :, columns] = answer[first:first + cap]

    back_copies, own_back = {}, {}
    order = list(range(1, outer)) + [0]
    for step in order:
        for hop in range(1, plane):
            peer = lax.rem(me + hop, plane)
            back_copies[step, hop] = remote(
                answers.at[step, peer], back.at[step, me],
                back_send.at[step, hop], back_recv.at[step, hop], near(peer),
            )
            back_copies[step, hop].start()
        own_back[step] = pltpu.make_async_copy(answers.at[step, me], back.at[step, me], own_sem.at[step])
        own_back[step].start()
    part_copies = {}
    total = hidden_ref[...].astype(jnp.float32)
    for step in order:
        own_back[step].wait()
        for hop in range(1, plane):
            back_copies[step, hop].wait_recv()
        arrived = jnp.concatenate([back[step, index] for index in range(plane)], axis=0)
        if step:
            high, low = route[step, slots:slots + toks, :slots], route[step, slots + toks:, :slots]
        else:
            high, low = route_ref[level, slots:slots + toks, :slots], route_ref[level, slots + toks:, :slots]
        mixed = jnp.dot(high, arrived, preferred_element_type=jnp.float32) + jnp.dot(
            low, arrived, preferred_element_type=jnp.float32
        )
        if step:
            partial[step] = mixed.astype(jnp.bfloat16)
            part_copies[step] = remote(
                partial.at[step], parts.at[step], part_send.at[step], part_recv.at[step], far(outer - step)
            )
            part_copies[step].start()
        else:
            total = total + mixed
    for step in range(1, outer):
        part_copies[step].wait_recv()
        total = total + parts[step].astype(jnp.float32)
    out_ref[...] = total
    for step in range(1, outer):
        route_copies[step].wait_send()
        far_copies[step].wait_send()
        part_copies[step].wait_send()
    for step in range(outer):
        for hop in range(1, plane):
            near_copies[step, hop].wait_send()
            back_copies[step, hop].wait_send()


def run_experts(normed, hidden, expert_gate, expert_down, route, shape):
    outer, plane, _, _, cap = shape
    toks, width = normed.shape
    ff = expert_gate.shape[2]
    count = outer * plane * cap
    dma = pltpu.SemaphoreType.DMA
    vmem = pl.BlockSpec(memory_space=pltpu.VMEM)
    hbm = pl.BlockSpec(memory_space=pl.ANY)
    low = jnp.bfloat16
    return pl.pallas_call(
        functools.partial(experts_kernel, shape),
        out_shape=jax.ShapeDtypeStruct((toks, width), jnp.float32),
        in_specs=[vmem, vmem, vmem, hbm, hbm],
        out_specs=vmem,
        scratch_shapes=[
            pltpu.VMEM((outer, toks, width), low),
            pltpu.VMEM(route.shape, low),
            pltpu.VMEM((outer, plane, cap, width), low),
            pltpu.VMEM((plane, outer, cap, width), low),
            pltpu.VMEM((count, width), low),
            pltpu.VMEM((count, ff), low),
            pltpu.VMEM((outer, plane, cap, width), low),
            pltpu.VMEM((outer, plane, cap, width), low),
            pltpu.VMEM((outer, toks, width), low),
            pltpu.VMEM((outer, toks, width), low),
            pltpu.VMEM(expert_gate.shape[1:], low),
            pltpu.VMEM(expert_down.shape[1:], low),
            dma((2,)), dma((outer,)), dma((outer,)), dma((outer,)), dma((outer,)),
            dma((outer, plane)), dma((outer, plane)), dma((outer,)),
            dma((outer, plane)), dma((outer, plane)), dma((outer,)), dma((outer,)),
        ],
        compiler_params=pltpu.CompilerParams(
            collective_id=2, has_side_effects=True, vmem_limit_bytes=60 * 1024 * 1024
        ),
    )(normed, hidden, route, expert_gate, expert_down).astype(low)


def routing(expert_ids, affinity, shape):
    outer, plane, _, _, cap = shape
    toks = expert_ids.shape[0]
    experts = outer * plane
    weight = route_scale * affinity / jnp.sum(affinity, axis=1, keepdims=True)
    named = expert_ids[:, :, None] == lax.broadcasted_iota(jnp.int32, (1, 1, experts), 2)
    chosen = jnp.sum(named.astype(jnp.int32), axis=1)
    weights = jnp.sum(jnp.where(named, weight[:, :, None], 0.0), axis=1)
    before = lax.broadcasted_iota(jnp.int32, (toks, toks, 1), 1) < lax.broadcasted_iota(
        jnp.int32, (toks, toks, 1), 0
    )
    rank = jnp.sum(jnp.where(before, chosen[None], 0), axis=1)
    rank = jnp.where(chosen > 0, rank, -1)
    in_slot = rank[:, :, None] == lax.broadcasted_iota(jnp.int32, (1, 1, cap), 2)
    in_slot = in_slot.reshape(toks, outer, plane * cap)
    spread = jnp.repeat(weights, cap, axis=1).reshape(toks, outer, plane * cap)
    spread = jnp.where(in_slot, spread, 0.0)
    high = spread.astype(jnp.bfloat16)
    rest = (spread - high.astype(jnp.float32)).astype(jnp.bfloat16)
    lanes = 128 * (-(-max(toks, plane * cap) // 128))

    def padded(array):
        return jnp.pad(array, ((0, 0), (0, 0), (0, lanes - array.shape[2])))

    pick = padded(in_slot.astype(jnp.bfloat16).transpose(1, 2, 0))
    return jnp.concatenate(
        [pick, padded(high.transpose(1, 0, 2)), padded(rest.transpose(1, 0, 2))], axis=1
    )


def solution(mesh):
    return jax.shard_map(
        per_device,
        mesh=mesh,
        in_specs=(
            P(("dp", "tp"), None),
            P(("dp", "tp"), None, None),
            P(("dp", "tp"), None),
            P(("dp", "tp"), None, None),
            P(("dp", "tp"), None, None),
            P(("dp", "tp")),
            P(None, "tp"),
            P("tp", None),
            P(),
            P(("dp", "tp"), None, None),
            P(("dp", "tp"), None, None),
            P(("dp", "tp"), None),
            P(("dp", "tp"), None),
        ),
        out_specs=P(("dp", "tp"), None),
        check_vma=False,
    )
```
